32 devices in a mesh: row: 8 (over y, x, core), col: 4 (over z).
Axes of the slice: x: 2, y: 2, z: 4, core: 2. Of those that a mesh axis runs over, the one named last changes fastest.
Arguments:
- right_sides: float32 [8, 8192, 128], P(None, ('row', 'col')), may hold values from -6 to 6
- factor_head: bfloat16 [8, 8192, 4, 1024], P(None, 'row', None, 'col'), may hold values from -0.1875 to 0.1875
- class_head: int32 [8, 8, 4], P(None, 'row'), may hold values from 0 to 2
- scale_head: float32 [8, 8, 4], P(None, 'row'), may hold values from 0.25 to 2
- inverse_head: float32 [4, 1024, 1024], P(None, 'col'), as said below
- factor_tail: bfloat16 [4, 1024, 8, 8192], P(None, 'col', None, 'row'), may hold values from -0.1875 to 0.1875
- class_tail: int32 [4, 8, 8], P(None, None, 'row'), may hold values from 0 to 2
- scale_tail: float32 [4, 8, 8], P(None, None, 'row'), may hold values from 0.25 to 2
- inverse_tail: float32 [4, 1024, 1024], P(None, None, 'col'), as said below
Outputs:
- solved_head: float32 [4, 1024, 128], P(None, 'col')
- solved_tail: float32 [4, 1024, 128], P(None, 'col')
- remainder: float32 [8, 8192, 128], P(None, ('row', 'col'))
The draws below stay inside these ranges and needn't reach their ends.
Inputs may be any that keep to these rules, and one draw needn't show every extreme that they name: `class_head`: 0, 1, 2 name the float32, bfloat16 and scaled bfloat16 classes. `class_tail`: 0, 1, 2 name the float32, bfloat16 and scaled bfloat16 classes. `inverse_head`: every tile is lower triangular with a diagonal of 1 to 2. `inverse_tail`: every tile is lower triangular with a diagonal of 1 to 2.
All inputs are finite; a program needn't handle non-finite values.
Results may differ from the reference program's by a relative error of at most 0.008.
Values sent between devices are 32-bit elements; how exact they have to be, the bound alone decides.
A program may use at most 128 MiB of HBM per device.

```python
import math
import jax
import jax.numpy as jnp
from jax import lax

TILE = 1024
SLOTS = 8
RHS = 128
WIN = 4
N_ROW = 8


def lower_inverse(key):
    first_key, second_key = jax.random.split(key)
    spread = jax.random.normal(first_key, (WIN, TILE, TILE), jnp.float32) * (0.7 / math.sqrt(TILE))
    diagonal = jnp.exp(jax.random.uniform(second_key, (WIN, TILE), jnp.float32, 0.0, math.log(2.0)))
    return jnp.tril(spread, -1) + jnp.eye(TILE, dtype=jnp.float32)[None, :, :] * diagonal[:, None, :]


def draw_inverse_head(key, part):
    return lower_inverse(jax.random.fold_in(key, 11))


def draw_inverse_tail(key, part):
    return lower_inverse(jax.random.fold_in(key, 23))


def with_ends(result, rng, low, top_value):
    spot = [jax.random.randint(jax.random.fold_in(rng, axis), (), 0, length) for axis, length in enumerate(result.shape)]
    widest = result.shape.index(max(result.shape))
    neighbour = spot[:widest] + [(spot[widest] + 1) % result.shape[widest]] + spot[widest + 1:]
    return result.at[tuple(spot)].set(low).at[tuple(neighbour)].set(top_value)


def block_scale(stream_key, shape, cuts, least, high):
    def one(axis_at, parts):
        steps = jax.random.uniform(jax.random.fold_in(jax.random.fold_in(stream_key, 6), axis_at), (parts,), jnp.float32, least / len(cuts), high / len(cuts))
        return jnp.repeat(jnp.exp(steps), shape[axis_at] // parts).reshape((-1,) + (1,) * (len(shape) - axis_at - 1))

    gain = one(*cuts[0])
    for cut in cuts[1:]:
        gain = gain * one(*cut)
    return gain


def bell_draw(key, shape, width, limit, shards=(), kind=jnp.bfloat16):
    values = jax.random.normal(key, shape, jnp.float32) * width
    if len(shards) > 0:
        values = block_scale(key, shape, shards, -0.22, 0.18) * values
    return jnp.clip(values, min=-limit, max=limit).astype(kind)


def setup_inputs(seed: int = 0) -> dict:
    seeds = jax.random.split(jax.random.key(seed), 10)
    right_sides = bell_draw(seeds[0], (SLOTS, N_ROW * TILE, RHS), 1.0, 6.0, ((1, 32),), jnp.float32)
    factor_head = bell_draw(seeds[1], (SLOTS, N_ROW * TILE, WIN, TILE), TILE ** -0.5, 0.1875, ((1, 8), (3, 4)))
    class_head = with_ends(jax.random.randint(seeds[2], (SLOTS, N_ROW, WIN), 0, 3), jax.random.fold_in(seeds[2], 1), 0, 2).astype(jnp.int32)
    scale_head = jnp.clip(jnp.exp(math.log(2.0) - 2.0794415 * jax.random.uniform(seeds[3], (SLOTS, N_ROW, WIN), jnp.float32) ** block_scale(seeds[3], (SLOTS, N_ROW, WIN), ((1, 8),), -0.2, 0.2)), 0.25, 2.0)
    inverse_head = draw_inverse_head(jax.random.fold_in(seeds[9], 71), 0)
    factor_tail = bell_draw(seeds[5], (WIN, TILE, SLOTS, N_ROW * TILE), TILE ** -0.5, 0.1875, ((1, 4), (3, 8)))
    class_tail = with_ends(jax.random.randint(seeds[6], (WIN, SLOTS, N_ROW), 0, 3), jax.random.fold_in(seeds[6], 1), 0, 2).astype(jnp.int32)
    scale_tail = jnp.clip(jnp.exp(math.log(2.0) - 2.0794415 * jax.random.uniform(seeds[7], (WIN, SLOTS, N_ROW), jnp.float32) ** block_scale(seeds[7], (WIN, SLOTS, N_ROW), ((2, 8),), -0.2, 0.2)), 0.25, 2.0)
    inverse_tail = draw_inverse_tail(jax.random.fold_in(seeds[9], 71), 0)
    return dict(right_sides=right_sides, factor_head=factor_head, class_head=class_head, scale_head=scale_head, inverse_head=inverse_head, factor_tail=factor_tail, class_tail=class_tail, scale_tail=scale_tail, inverse_tail=inverse_tail)


def tile_terms(stored, classes, scales, piece, form):
    exact_piece = piece
    short_piece = piece.astype(jnp.bfloat16).astype(jnp.float32)
    wide = stored.astype(jnp.float32)
    exact_term = jnp.einsum(form, wide, exact_piece, precision=lax.Precision.HIGHEST)
    short_term = jnp.einsum(form, wide, short_piece, precision=lax.Precision.HIGHEST)
    classes = classes[:, None, None]
    scales = scales[:, None, None]
    return jnp.where(classes == 0, exact_term, jnp.where(classes == 1, short_term, scales * short_term))


def reference(right_sides, factor_head, class_head, scale_head, inverse_head, factor_tail, class_tail, scale_tail, inverse_tail):
    ntiles = SLOTS * N_ROW
    state = right_sides.reshape(SLOTS, N_ROW, TILE, RHS)
    tile_ids = jnp.arange(SLOTS, dtype=jnp.int32)[:, None] * N_ROW + jnp.arange(N_ROW, dtype=jnp.int32)[None, :]
    head_tiles = factor_head.reshape(SLOTS, N_ROW, TILE, WIN, TILE)
    heads = []
    for step in range(WIN):
        slot_k, row_k = divmod(step, N_ROW)
        solved = jnp.dot(inverse_head[step], state[slot_k, row_k], precision=lax.Precision.HIGHEST, preferred_element_type=jnp.float32)
        heads.append(solved)

        def one_slot(args):
            stored, classes, scales = args
            return tile_terms(stored, classes, scales, solved, "rab,bn->ran")

        terms = lax.map(one_slot, (head_tiles[:, :, :, step, :], class_head[:, :, step], scale_head[:, :, step]))
        active = (tile_ids > step)[:, :, None, None]
        state = state - jnp.where(active, terms, jnp.float32(0.0))
    tail_tiles = factor_tail.reshape(WIN, TILE, SLOTS, N_ROW, TILE)
    tails = [None] * WIN
    for step in range(WIN):
        target = ntiles - 1 - step
        window = WIN - 1 - step
        slot_j, row_j = divmod(target, N_ROW)
        solved = jnp.dot(inverse_tail[window].T, state[slot_j, row_j], precision=lax.Precision.HIGHEST, preferred_element_type=jnp.float32)
        tails[window] = solved
        stored_all = jnp.moveaxis(tail_tiles[window], 1, 0)

        def one_slot_back(args):
            stored, classes, scales = args
            return tile_terms(stored, classes, scales, solved, "arb,an->rbn")

        terms = lax.map(one_slot_back, (stored_all, class_tail[window], scale_tail[window]))
        active = (tile_ids < target)[:, :, None, None]
        state = state - jnp.where(active, terms, jnp.float32(0.0))
    return jnp.stack(heads), jnp.stack(tails), state.reshape(SLOTS, N_ROW * TILE, RHS)
```

```python
import functools

import jax
import jax.numpy as jnp
from jax import lax
from jax.experimental import pallas as pl
from jax.experimental.pallas import tpu as pltpu
from jax.sharding import PartitionSpec as P

MESH = pl.DeviceIdType.MESH


def chain_kernel(
    n_row,
    n_col,
    coef_ref,
    right_ref,
    tiles_ref,
    inverse_head_ref,
    inverse_tail_ref,
    solved_out,
    solved,
    pair,
    part,
    sums,
    value,
    sum_send,
    sum_recv,
    value_send,
    value_recv,
    solved_send,
    solved_recv,
):
    window, share = inverse_head_ref.shape[0], inverse_head_ref.shape[1]
    columns = right_ref.shape[2]
    row, col = lax.axis_index("row"), lax.axis_index("col")

    def other_col(shift):
        return lax.rem(col + shift + n_col, n_col)

    def other_row(shift):
        return lax.rem(row + shift + n_row, n_row)

    barrier = pltpu.get_barrier_semaphore()
    for shift in range(1, n_col):
        pl.semaphore_signal(
            barrier, inc=1, device_id=(row, other_col(shift)), device_id_type=MESH
        )
    for shift in range(1, n_row):
        pl.semaphore_signal(
            barrier, inc=1, device_id=(other_row(shift), col), device_id_type=MESH
        )
    part[...] = jnp.zeros_like(part)
    pl.semaphore_wait(barrier, n_col + n_row - 2)

    def sum_copy(phase, shift):
        peer = other_col(shift)
        return pltpu.make_async_remote_copy(
            src_ref=part.at[phase, peer],
            dst_ref=sums.at[phase, shift - 1],
            send_sem=sum_send.at[phase, shift - 1],
            recv_sem=sum_recv.at[phase, shift - 1],
            device_id=(row, peer),
            device_id_type=MESH,
        )

    def value_copy(phase, shift):
        return pltpu.make_async_remote_copy(
            src_ref=value.at[phase, col],
            dst_ref=value.at[phase, col],
            send_sem=value_send.at[phase, shift - 1],
            recv_sem=value_recv.at[phase, shift - 1],
            device_id=(row, other_col(shift)),
            device_id_type=MESH,
        )

    def value_landed(phase, shift):
        source = other_col(-shift)
        return pltpu.make_async_remote_copy(
            src_ref=value.at[phase, source],
            dst_ref=value.at[phase, source],
            send_sem=value_send.at[phase, shift - 1],
            recv_sem=value_recv.at[phase, shift - 1],
            device_id=(row, source),
            device_id_type=MESH,
        )

    def solved_copy(index, shift):
        return pltpu.make_async_remote_copy(
            src_ref=solved.at[index],
            dst_ref=solved.at[index],
            send_sem=solved_send.at[index, shift - 1],
            recv_sem=solved_recv.at[index],
            device_id=(other_row(shift if index < window else -shift), col),
            device_id_type=MESH,
        )

    owners = [step for step in range(window)]
    owners += [n_row - 1 - step for step in range(window)]
    for index in range(2 * window):
        phase, step = divmod(index, window)
        position = step if phase == 0 else window - 1 - step
        inverse_ref = inverse_head_ref if phase == 0 else inverse_tail_ref

        @pl.when(row == owners[index])
        def _(index=index, phase=phase, position=position, inverse_ref=inverse_ref):
            total = right_ref[phase]
            if index > 0:
                for shift in range(1, n_col):
                    sum_copy(phase, shift).start()
                total = total - part[phase, col]
                for shift in range(1, n_col):
                    sum_copy(phase, shift).wait_recv()
                    total = total - sums[phase, shift - 1]
            value[phase, col] = total
            for shift in range(1, n_col):
                value_copy(phase, shift).start()

            def times(source):
                start = pl.multiple_of(source * share, share)
                return jnp.dot(
                    inverse_ref[position, :, pl.ds(start, share)],
                    value[phase, source],
                    precision=lax.Precision.HIGHEST,
                    preferred_element_type=jnp.float32,
                )

            result = times(col)
            for shift in range(1, n_col):
                value_landed(phase, shift).wait_recv()
                result = result + times(other_col(-shift))
            solved[index] = result
            for shift in range(1, n_row):
                solved_copy(index, shift).start()
            if index > 0:
                for shift in range(1, n_col):
                    sum_copy(phase, shift).wait_send()

        @pl.when(row != owners[index])
        def _(index=index):
            solved_copy(index, 1).wait_recv()

        if index == 2 * window - 1:
            break
        full = solved[index]
        high = full.astype(jnp.bfloat16)
        pair[:, :columns] = high
        pair[:, columns:] = (full - high.astype(jnp.float32)).astype(jnp.bfloat16)
        for kind in (0, 1) if phase == 0 else (2,):
            target = 0 if kind == 0 else 1
            high_coef = coef_ref[0, kind, position]
            low_coef = coef_ref[1, kind, position]

            def add_block(block, carry, kind=kind, target=target, high_coef=high_coef, low_coef=low_coef, position=position):
                product = jnp.dot(
                    tiles_ref[kind, position, block],
                    pair[...],
                    preferred_element_type=jnp.float32,
                )
                part[target, block] += (
                    high_coef * product[:, :columns] + low_coef * product[:, columns:]
                )
                return carry

            lax.fori_loop(0, n_col, add_block, 0)

    solved_out[...] = solved[...]
    for index in range(2 * window):

        @pl.when(row == owners[index])
        def _(index=index):
            for shift in range(1, n_col):
                value_copy(index // window, shift).wait_send()
            for shift in range(1, n_row):
                solved_copy(index, shift).wait_send()


def solve_chain(coefs, rights, tiles, inverse_head, inverse_tail, n_row, n_col):
    window, share = inverse_head.shape[:2]
    columns = rights.shape[2]
    piece = (share, columns)
    vmem = pl.BlockSpec(memory_space=pltpu.VMEM)
    dma = pltpu.SemaphoreType.DMA
    return pl.pallas_call(
        functools.partial(chain_kernel, n_row, n_col),
        out_shape=jax.ShapeDtypeStruct((2 * window,) + piece, jnp.float32),
        in_specs=[pl.BlockSpec(memory_space=pltpu.SMEM)] + [vmem] * 4,
        out_specs=vmem,
        scratch_shapes=[
            pltpu.VMEM((2 * window,) + piece, jnp.float32),
            pltpu.VMEM((share, 2 * columns), jnp.bfloat16),
            pltpu.VMEM((2, n_col) + piece, jnp.float32),
            pltpu.VMEM((2, n_col - 1) + piece, jnp.float32),
            pltpu.VMEM((2, n_col) + piece, jnp.float32),
            dma((2, n_col - 1)),
            dma((2, n_col - 1)),
            dma((2, n_col - 1)),
            dma((2, n_col - 1)),
            dma((2 * window, n_row - 1)),
            dma((2 * window,)),
        ],
        compiler_params=pltpu.CompilerParams(
            collective_id=0, has_side_effects=True, vmem_limit_bytes=40 * 2**20
        ),
    )(coefs, rights, tiles, inverse_head, inverse_tail)


def weighted_pairs(solved, classes, scales, active):
    classes, scales, active = (
        jnp.transpose(x)[:, :, None, None] for x in (classes, scales, active)
    )
    full = solved[None]
    short = lax.reduce_precision(full, 8, 7)
    piece = jnp.where(classes == 0, full, jnp.where(classes == 1, short, scales * short))
    piece = jnp.where(active, piece, jnp.float32(0.0))
    high = lax.reduce_precision(piece, 8, 7)
    return jnp.concatenate([high, piece - high], axis=3).astype(jnp.bfloat16)


def on_device(
    right_sides,
    factor_head,
    class_head,
    scale_head,
    inverse_head,
    factor_tail,
    class_tail,
    scale_tail,
    inverse_tail,
):
    n_row, n_col = lax.axis_size("row"), lax.axis_size("col")
    slots, share, columns = right_sides.shape
    ntiles = slots * n_row
    window = inverse_head.shape[0]
    tile_ids = jnp.arange(slots, dtype=jnp.int32) * n_row + lax.axis_index("row")
    steps = jnp.arange(window, dtype=jnp.int32)[:, None]
    head_class, head_scale = class_head[:, 0].T, scale_head[:, 0].T
    tail_class, tail_scale = class_tail[:, :, 0], scale_tail[:, :, 0]
    head_active = tile_ids[None, :] > steps
    tail_active = tile_ids[None, :] < ntiles - window + steps

    def coefs_of(classes, scales, active):
        high = jnp.where(active, jnp.where(classes == 2, scales, 1.0), 0.0)
        low = jnp.where(active, jnp.where(classes == 0, 1.0, 0.0), 0.0)
        return jnp.stack([high, low]).astype(jnp.float32)

    head_coefs = coefs_of(head_class, head_scale, head_active)
    tail_coefs = coefs_of(tail_class, tail_scale, tail_active)
    coefs = jnp.stack([head_coefs[:, :, 0], head_coefs[:, :, -1], tail_coefs[:, :, -1]], axis=1)
    tiles = jnp.stack(
        [
            jnp.transpose(factor_head[0], (1, 0, 2)),
            jnp.transpose(factor_head[-1], (1, 0, 2)),
            jnp.transpose(factor_tail[:, :, -1], (0, 2, 1)),
        ]
    ).reshape(3, window, n_col, share, share)
    rights = jnp.stack([right_sides[0], right_sides[-1]])
    solved = solve_chain(
        coefs,
        rights,
        tiles,
        inverse_head,
        jnp.transpose(inverse_tail, (0, 2, 1)),
        n_row,
        n_col,
    )
    heads, tails = solved[:window], solved[window:][::-1]
    head_pairs = weighted_pairs(heads, head_class, head_scale, head_active)
    tail_pairs = weighted_pairs(tails, tail_class, tail_scale, tail_active)
    updates = jnp.einsum(
        "lakb,lkbn->lan", factor_head, head_pairs, preferred_element_type=jnp.float32
    ) + jnp.einsum(
        "walb,lwan->lbn", factor_tail, tail_pairs, preferred_element_type=jnp.float32
    )
    updates = updates[:, :, :columns] + updates[:, :, columns:]
    summed = lax.psum_scatter(updates, "col", scatter_dimension=1, tiled=True)
    return heads, tails, right_sides - summed


def solution(mesh):
    return jax.shard_map(
        on_device,
        mesh=mesh,
        in_specs=(
            P(None, ("row", "col"), None),
            P(None, "row", None, "col"),
            P(None, "row", None),
            P(None, "row", None),
            P(None, "col", None),
            P(None, "col", None, "row"),
            P(None, None, "row"),
            P(None, None, "row"),
            P(None, None, "col"),
        ),
        out_specs=(P(None, "col", None), P(None, "col", None), P(None, ("row", "col"), None)),
        check_vma=False,
    )
```
